32 devices in a mesh: grp: 4 (over x, core), shard: 8 (over z, y).
Axes of the slice: x: 2, y: 2, z: 4, core: 2. Of those that a mesh axis runs over, the one named last changes fastest.
Arguments:
- tokens: bfloat16 [1024, 1280], P('shard'), may hold values from -6 to 6
- fc1_mean: float32 [5120, 1280], P('shard'), may hold values from -0.15625 to 0.15625
- fc1_variance: float32 [5120, 1280], P('shard'), may hold values from 1e-05 to 0.001
- fc1_deviation: bfloat16 [20, 5120, 1280], P(None, 'shard'), may hold values from -0.19921875 to 0.19921875
- fc2_mean: float32 [1280, 5120], P(None, 'shard'), may hold values from -0.078125 to 0.078125
- fc2_variance: float32 [1280, 5120], P(None, 'shard'), may hold values from 2.5e-06 to 0.00025
- fc2_deviation: bfloat16 [20, 1280, 5120], P(None, None, 'shard'), may hold values from -0.099609375 to 0.099609375
- noise_fc1: bfloat16 [8, 5120, 1280], P('grp', 'shard'), may hold values from -6 to 6
- noise_fc2: bfloat16 [8, 1280, 5120], P('grp', None, 'shard'), may hold values from -6 to 6
- noise_low: float32 [8, 20], P('grp'), may hold values from -4 to 4
Outputs:
- prediction: bfloat16 [1024, 1280], P('shard', 'grp')
The draws below stay inside these ranges and needn't reach their ends.
All inputs are finite; a program needn't handle non-finite values.
Results may differ from the reference program's by a relative error of at most 0.013.
Values may be sent and summed in bfloat16 or wider, within the bound.
A program may use at most 256 MiB of HBM per device.

```python
import math
import jax
import jax.numpy as jnp
from jax import lax

D = 1280
FF = 5120
K = 20
SAMPLES = 8
TOKENS = 1024


def block_levels(own_key, dims, cuts, least, largest):
    gain, own = 1.0, jax.random.fold_in(own_key, 6)
    for axis_at, parts in cuts:
        steps = jnp.exp(jax.random.uniform(jax.random.fold_in(own, axis_at), (parts,), jnp.float32, least / len(cuts), largest / len(cuts)))
        gain = gain * jnp.repeat(steps, dims[axis_at] // parts).reshape([-1 if axis == axis_at else 1 for axis in range(len(dims))])
    return gain


def bell_draw(own_key, dims, scale, most, split=(), kind=jnp.bfloat16):
    values = scale * jax.random.normal(own_key, dims, jnp.float32)
    if split:
        values = values * block_levels(own_key, dims, split, -0.22, 0.18)
    return jnp.clip(values, -most, most).astype(kind)


def setup_inputs(seed: int = 0) -> dict:
    arg_keys = jax.random.split(jax.random.key(seed), 11)
    return {
        "tokens": bell_draw(arg_keys[0], (TOKENS, D), 1.0, 6.0, ((0, 8),)),
        "fc1_mean": bell_draw(arg_keys[1], (FF, D), D ** -0.5, 0.15625, ((0, 8),), jnp.float32),
        "fc1_variance": jnp.clip(jnp.exp(math.log(0.001) - 4.6051703 * jax.random.uniform(arg_keys[2], (FF, D), jnp.float32) ** block_levels(arg_keys[2], (FF, D), ((0, 8),), -0.2, 0.2)), 9.999999747378752e-06, 0.001),
        "fc1_deviation": bell_draw(arg_keys[3], (K, FF, D), 0.03, 0.19921875, ((1, 8),)),
        "fc2_mean": bell_draw(arg_keys[4], (D, FF), FF ** -0.5, 0.078125, ((1, 8),), jnp.float32),
        "fc2_variance": jnp.clip(jnp.exp(math.log(0.00025) - 4.6051703 * jax.random.uniform(arg_keys[5], (D, FF), jnp.float32) ** block_levels(arg_keys[5], (D, FF), ((1, 8),), -0.2, 0.2)), 2.499999936844688e-06, 0.00025),
        "fc2_deviation": bell_draw(arg_keys[6], (K, D, FF), 0.015, 0.099609375, ((2, 8),)),
        "noise_fc1": bell_draw(arg_keys[7], (SAMPLES, FF, D), 1.0, 6.0, ((0, 4), (1, 8))),
        "noise_fc2": bell_draw(arg_keys[8], (SAMPLES, D, FF), 1.0, 6.0, ((0, 4), (2, 8))),
        "noise_low": bell_draw(arg_keys[9], (SAMPLES, K), 1.0, 4.0, ((0, 4),), jnp.float32),
    }


def sample_weights(moment_mean, moment_variance, deviation, noise_diag, low_half):
    columns = deviation.shape[0]
    flattened = deviation.reshape(columns, -1)
    low_rank = jnp.dot(low_half, flattened, preferred_element_type=jnp.float32)
    low_rank = low_rank.reshape((low_half.shape[0],) + moment_mean.shape)
    sampled = moment_mean[None] + jnp.sqrt(moment_variance)[None] * noise_diag.astype(jnp.float32)
    sampled = sampled + low_rank / math.sqrt(2.0 * (columns - 1))
    return sampled.astype(jnp.bfloat16)

def reference(tokens, fc1_mean, fc1_variance, fc1_deviation, fc2_mean, fc2_variance, fc2_deviation, noise_fc1, noise_fc2, noise_low):
    low_half = noise_low.astype(jnp.bfloat16)
    up_weights = sample_weights(fc1_mean, fc1_variance, fc1_deviation, noise_fc1, low_half)
    down_weights = sample_weights(fc2_mean, fc2_variance, fc2_deviation, noise_fc2, low_half)

    def accumulate(running, weight_pair):
        first_w, second_w = weight_pair
        preact = jnp.dot(tokens, first_w.T, preferred_element_type=jnp.float32)
        hidden = jax.nn.gelu(preact, approximate=False).astype(jnp.bfloat16)
        return (running + jnp.dot(hidden, second_w.T, preferred_element_type=jnp.float32), None)
    start_sum = jnp.zeros((tokens.shape[0], tokens.shape[1]), jnp.float32)
    summed, _ = lax.scan(accumulate, start_sum, (up_weights, down_weights))
    return (summed / SAMPLES).astype(jnp.bfloat16)
```

```python
import functools
import math

import jax
import jax.numpy as jnp
from jax import lax
from jax.experimental import pallas as pl
from jax.experimental.pallas import tpu as pltpu
from jax.sharding import PartitionSpec as P

UNIT = 32


def from_partner(value, axis, mask):
    pairs = [(source, source ^ mask) for source in range(lax.axis_size(axis))]
    return lax.ppermute(value, axis, pairs)


def sample_kernel(scale, unit, order_ref, spread_ref, mean_ref, variance_ref, deviation_ref, noise_ref, out_ref):
    samples = noise_ref.shape[0]
    columns, rows, width = deviation_ref.shape

    def step(i, carry):
        at = pl.ds(pl.multiple_of(i * unit, unit), unit)
        stacked = deviation_ref[:, at, :].reshape(columns * unit, width)
        low_rank = jnp.dot(spread_ref[...], stacked, preferred_element_type=jnp.float32)
        mean = mean_ref[at, :]
        std = jnp.sqrt(variance_ref[at, :])
        for s in range(samples):
            part = low_rank[s * unit : (s + 1) * unit]
            value = mean + std * noise_ref[s, at, :].astype(jnp.float32) + part * scale
            out_ref[s, at, :] = value.astype(out_ref.dtype)
        return carry

    lax.fori_loop(0, rows // unit, step, 0)


def sample_weights(order, parts, mean, variance, deviation, noise, low_half, name):
    columns, rows, width = deviation.shape
    samples = noise.shape[0]
    per_part = rows // parts
    unit = math.gcd(UNIT, per_part)
    block = max(
        b
        for b in range(unit, per_part + 1, unit)
        if per_part % b == 0 and (b == unit or columns * b * width * 2 <= 4500000)
    )
    steps = per_part // block
    eye = jnp.eye(unit, dtype=jnp.bfloat16)
    spread = (low_half[:, None, :, None] * eye[None, :, None, :]).reshape(samples * unit, columns * unit)

    def source(i, order):
        return order[i // steps] * steps + i % steps

    count = rows * width
    return pl.pallas_call(
        functools.partial(sample_kernel, 1.0 / math.sqrt(2.0 * (columns - 1)), unit),
        grid_spec=pltpu.PrefetchScalarGridSpec(
            num_scalar_prefetch=1,
            grid=(parts * steps,),
            in_specs=[
                pl.BlockSpec(spread.shape, lambda i, o: (0, 0)),
                pl.BlockSpec((block, width), lambda i, o: (source(i, o), 0)),
                pl.BlockSpec((block, width), lambda i, o: (source(i, o), 0)),
                pl.BlockSpec((columns, block, width), lambda i, o: (0, source(i, o), 0)),
                pl.BlockSpec((samples, block, width), lambda i, o: (0, source(i, o), 0)),
            ],
            out_specs=pl.BlockSpec((samples, block, width), lambda i, o: (0, i, 0)),
        ),
        out_shape=jax.ShapeDtypeStruct((samples, rows, width), jnp.bfloat16),
        cost_estimate=pl.CostEstimate(
            flops=2 * count * columns * samples,
            bytes_accessed=count * (2 * columns + 8 + 4 * samples),
            transcendentals=count,
        ),
        compiler_params=pltpu.CompilerParams(
            dimension_semantics=("arbitrary",), vmem_limit_bytes=60 * 1024 * 1024
        ),
        name=name,
    )(order, spread, mean, variance, deviation, noise)


def mlp_kernel(core_ref, own_ref, other_ref, up_ref, down_ref, out_ref):
    half = own_ref.shape[1]
    parts, _, piece = out_ref.shape
    core = core_ref[0]
    own_at = pl.ds(pl.multiple_of(core * half, half), half)
    other_at = pl.ds(pl.multiple_of((1 - core) * half, half), half)
    across = (((1,), (1,)), ((), ()))
    total = None
    for s in range(up_ref.shape[0]):
        preact = lax.dot_general(own_ref[...], up_ref[s, :, own_at], across, preferred_element_type=jnp.float32)
        preact += lax.dot_general(other_ref[...], up_ref[s, :, other_at], across, preferred_element_type=jnp.float32)
        hidden = (0.5 * preact * (1.0 + lax.erf(preact * math.sqrt(0.5)))).astype(jnp.bfloat16)
        term = lax.dot_general(hidden, down_ref[s], across, preferred_element_type=jnp.float32)
        total = term if total is None else total + term
    for p in range(parts):
        out_ref[p] = total[:, p * piece : (p + 1) * piece].astype(out_ref.dtype)


def mlp(core, own, other, up, down, parts):
    tokens, half = own.shape
    samples, hidden, width = up.shape
    block = min(256, tokens)
    piece = width // parts
    return pl.pallas_call(
        mlp_kernel,
        grid_spec=pltpu.PrefetchScalarGridSpec(
            num_scalar_prefetch=1,
            grid=(tokens // block,),
            in_specs=[
                pl.BlockSpec((block, half), lambda i, c: (i, 0)),
                pl.BlockSpec((block, half), lambda i, c: (i, 0)),
                pl.BlockSpec(up.shape, lambda i, c: (0, 0, 0)),
                pl.BlockSpec(down.shape, lambda i, c: (0, 0, 0)),
            ],
            out_specs=pl.BlockSpec((parts, block, piece), lambda i, c: (0, i, 0)),
        ),
        out_shape=jax.ShapeDtypeStruct((parts, tokens, piece), jnp.bfloat16),
        cost_estimate=pl.CostEstimate(
            flops=4 * tokens * samples * hidden * width,
            bytes_accessed=2 * (2 * tokens * width + 2 * samples * hidden * width),
            transcendentals=tokens * samples * hidden,
        ),
        compiler_params=pltpu.CompilerParams(
            dimension_semantics=("arbitrary",), vmem_limit_bytes=60 * 1024 * 1024
        ),
        name="mlp",
    )(core, own, other, up, down)


def fold(value, axis, mask, dim):
    kept = lax.index_in_dim(value, 0, dim, keepdims=True)
    sent = lax.index_in_dim(value, 1, dim, keepdims=True).astype(jnp.bfloat16)
    return kept.astype(jnp.float32) + from_partner(sent, axis, mask).astype(jnp.float32)


def body(
    tokens,
    fc1_mean,
    fc1_variance,
    fc1_deviation,
    fc2_mean,
    fc2_variance,
    fc2_deviation,
    noise_fc1,
    noise_fc2,
    noise_low,
):
    low_half = noise_low.astype(jnp.bfloat16)
    groups = lax.axis_size("grp")
    shard_count = lax.axis_size("shard")
    samples = noise_fc1.shape[0] * groups
    hid_ways = min(8, shard_count)
    low_bits = (shard_count // hid_ways).bit_length() - 1
    tok_bits = hid_ways.bit_length() - 1
    grp_bits = groups.bit_length() - 1
    position = lax.axis_index("shard")
    group = lax.axis_index("grp")
    core = group % 2
    rows, width = tokens.shape
    half = width // 2

    mine = lax.dynamic_slice_in_dim(tokens, core * half, half, 1)
    gathered = [mine] + [from_partner(mine, "shard", m << low_bits) for m in range(1, hid_ways)]

    order = jnp.bitwise_xor(jnp.arange(groups, dtype=jnp.int32), group.astype(jnp.int32))
    whole = jnp.zeros((1,), jnp.int32)
    up = sample_weights(whole, 1, fc1_mean, fc1_variance, fc1_deviation, noise_fc1, low_half, "sample_up")
    down = sample_weights(order, groups, fc2_mean, fc2_variance, fc2_deviation, noise_fc2, low_half, "sample_down")
    for bit in range(low_bits):
        upper = position >> bit & 1 == 1
        partner = from_partner(up, "shard", 1 << bit)
        up = jnp.where(upper, jnp.concatenate([partner, up], 1), jnp.concatenate([up, partner], 1))
        partner = from_partner(down, "shard", 1 << bit)
        down = jnp.where(upper, jnp.concatenate([partner, down], 2), jnp.concatenate([down, partner], 2))

    gathered, up, down = lax.optimization_barrier((gathered, up, down))
    own = jnp.concatenate(gathered, 0)
    other = from_partner(own, "grp", 1)
    partial = mlp(core.astype(jnp.int32).reshape(1), own, other, up, down, groups)

    piece = width // groups
    value = partial.reshape((2,) * grp_bits + (2,) * tok_bits + (2, rows // 2, piece))
    value = fold(value, "grp", 1, grp_bits - 1)
    grp_steps = [("grp", 1 << b, grp_bits - 1 - b) for b in range(1, grp_bits)]
    shard_steps = [("shard", 1 << (low_bits + b), grp_bits + tok_bits - 1 - b) for b in range(tok_bits)]
    first, second, rest = grp_steps, shard_steps[:1], shard_steps[:0:-1]
    done = []
    for stream, steps in enumerate((first + second + rest, second + first + rest)):
        part = lax.index_in_dim(value, stream, grp_bits + tok_bits, keepdims=False)
        for axis, mask, dim in steps:
            part = fold(part, axis, mask, dim)
        done.append(part.reshape(rows // 2, piece))
    return (jnp.concatenate(done, 0) / samples).astype(jnp.bfloat16)


def solution(mesh):
    placed = (
        P("shard", None),
        P("shard", None),
        P("shard", None),
        P(None, "shard", None),
        P(None, "shard"),
        P(None, "shard"),
        P(None, None, "shard"),
        P("grp", "shard", None),
        P("grp", None, "shard"),
        P("grp", None),
    )
    return jax.shard_map(
        body, mesh=mesh, in_specs=placed, out_specs=P("shard", "grp"), check_vma=False
    )
```
